512 devices in a mesh: brick: 128 (over x, z, core), chan: 4 (over y).
Axes of the slice: x: 4, y: 4, z: 16, core: 2. Of those that a mesh axis runs over, the one named last changes fastest.
Arguments:
- features: bfloat16 [512, 128, 512], P('brick', 'chan'), may hold values from -6 to 6
- fine_links: int32 [512, 26], P('brick'), may hold values from -1 to 511, as said below
- coarse_links: int32 [256, 26], P('brick'), may hold values from -1 to 255, as said below
- parents: int32 [512], P('brick'), may hold values from 0 to 2047, as said below
- down_weight: bfloat16 [8, 128, 128], P(None, None, 'chan'), may hold values from -0.1875 to 0.1875
- coarse_weight: bfloat16 [27, 128, 128], P(None, 'chan'), may hold values from -0.109375 to 0.109375
- up_weight: bfloat16 [8, 128, 128], P(None, 'chan'), may hold values from -0.5 to 0.5
- fine_weight: bfloat16 [27, 128, 128], P(None, 'chan'), may hold values from -0.109375 to 0.109375
- coarse_bias: float32 [128], P('chan'), may hold values from -3 to 3
- fine_bias: float32 [128], P('chan'), may hold values from -3 to 3
Outputs:
- refined: bfloat16 [512, 128, 512], P('brick', 'chan')
The draws below stay inside these ranges and needn't reach their ends.
Inputs may be any that keep to these rules, and one draw needn't show every extreme that they name: `fine_links`: A fine brick's index is its owner times 4 plus its place there; the owner of fine brick b is b // 4. Among the rows of one owner's bricks, at most 1 of the entries in columns 0 to 5 name bricks of any one owner, and at most 1 of the entries in columns 6 to 25 do. `coarse_links`: A coarse brick's index is its owner times 2 plus its place there. Among the rows of one owner's coarse bricks, at most 1 of the entries in columns 0 to 5 name coarse bricks of any one owner, and at most 1 of the entries in columns 6 to 25 do. parents[b] // 8 is a coarse brick; at most 1 of one owner's fine bricks have parents on any one owner.
All inputs are finite; a program needn't handle non-finite values.
Results may differ from the reference program's by a relative error of at most 0.0059.
Values may be sent and summed in bfloat16 or wider, within the bound.
A program may use at most 64 MiB of HBM per device.

```python
import jax
import jax.numpy as jnp
from jax import lax

C = 128
EDGE = 8
BR_DEV = 4
CBR_DEV = 2
BRICKS = 512
N_BRICK = 128


def owner_table(seed_key, item_total, owner_total, sparse):
    capacity = -(-item_total // owner_total)
    hot_owner = jax.random.randint(jax.random.fold_in(seed_key, 7), (), 0, owner_total)

    def one_device(device):
        local_key = jax.random.fold_in(seed_key, 100 + device)
        ranking = jax.random.permutation(jax.random.fold_in(local_key, 1), item_total).astype(jnp.int32)
        groups = ranking // capacity
        shuffled = jax.random.permutation(jax.random.fold_in(local_key, 2), owner_total - 1).astype(jnp.int32)
        offsets = jnp.concatenate([jnp.zeros((1,), jnp.int32), 1 + shuffled])
        target = (hot_owner + offsets[groups]) % owner_total
        coin_flip = jax.random.randint(jax.random.fold_in(local_key, 3), (item_total,), 0, 8)
        return jnp.where((groups == 0) | (coin_flip < sparse), target, -1).astype(jnp.int32)
    return jax.vmap(one_device)(jnp.arange(owner_total, dtype=jnp.int32))


def linked(seed_key, per_owner):
    face_owner = owner_table(jax.random.fold_in(seed_key, 1), 6 * per_owner, N_BRICK, 7)
    rim_owner = owner_table(jax.random.fold_in(seed_key, 2), 20 * per_owner, N_BRICK, 7)
    face_slot = jax.random.randint(jax.random.fold_in(seed_key, 3), face_owner.shape, 0, per_owner)
    rim_slot = jax.random.randint(jax.random.fold_in(seed_key, 4), rim_owner.shape, 0, per_owner)
    face_ids = jnp.where(face_owner >= 0, face_owner * per_owner + face_slot, -1).reshape(N_BRICK, per_owner, 6)
    rim_ids = jnp.where(rim_owner >= 0, rim_owner * per_owner + rim_slot, -1).reshape(N_BRICK, per_owner, 20)
    return jnp.concatenate([face_ids, rim_ids], axis=2).reshape(N_BRICK * per_owner, 26).astype(jnp.int32)


def draw_fine_links(key, part):
    return linked(jax.random.fold_in(key, 11), BR_DEV)


def draw_coarse_links(key, part):
    return linked(jax.random.fold_in(key, 12), CBR_DEV)


def draw_parents(key, part):
    seed_key = jax.random.fold_in(key, 13)
    owners = owner_table(jax.random.fold_in(seed_key, 1), BR_DEV, N_BRICK, 8)
    slot_draw = jax.random.randint(jax.random.fold_in(seed_key, 2), owners.shape, 0, CBR_DEV)
    octant = jax.random.randint(jax.random.fold_in(seed_key, 3), owners.shape, 0, 8)
    return ((owners * CBR_DEV + slot_draw) * 8 + octant).reshape(-1).astype(jnp.int32)


def level_of(stream_key, dims, cuts, least, high):
    def one(position, blocks):
        heights = jax.random.uniform(jax.random.fold_in(jax.random.fold_in(stream_key, 6), position), (blocks,), jnp.float32, least / len(cuts), high / len(cuts))
        return jnp.repeat(jnp.exp(heights), dims[position] // blocks).reshape((-1,) + (1,) * (len(dims) - position - 1))

    level = one(*cuts[0])
    for cut in cuts[1:]:
        level = level * one(*cut)
    return level


def scatter_about(rng, shape, spread, limit, shards=(), kind=jnp.bfloat16):
    level = level_of(rng, shape, shards, -0.22, 0.18) if shards else 1.0
    drawn = jax.random.normal(rng, shape, jnp.float32) * spread * level
    return jnp.minimum(jnp.maximum(drawn, -limit), limit).astype(kind)


def setup_inputs(seed: int = 0) -> dict:
    keys = jax.random.split(jax.random.key(seed), 11)
    features = scatter_about(keys[0], (BRICKS, C, EDGE ** 3), 1.0, 6.0, ((0, 128), (1, 4)))
    fine_links = draw_fine_links(jax.random.fold_in(keys[10], 71), 0)
    coarse_links = draw_coarse_links(jax.random.fold_in(keys[10], 71), 0)
    parents = draw_parents(jax.random.fold_in(keys[10], 71), 0)
    down_weight = scatter_about(keys[4], (8, C, C), (8 * C) ** -0.5, 0.1875, ((2, 4),))
    coarse_weight = scatter_about(keys[5], (27, C, C), (27 * C) ** -0.5, 0.109375, ((1, 4),))
    up_weight = scatter_about(keys[6], (8, C, C), C ** -0.5, 0.5, ((1, 4),))
    fine_weight = scatter_about(keys[7], (27, C, C), (27 * C) ** -0.5, 0.109375, ((1, 4),))
    coarse_bias = scatter_about(keys[8], (C,), 0.5, 3.0, ((0, 4),), jnp.float32)
    fine_bias = scatter_about(keys[9], (C,), 0.5, 3.0, ((0, 4),), jnp.float32)
    return dict(features=features, fine_links=fine_links, coarse_links=coarse_links, parents=parents, down_weight=down_weight, coarse_weight=coarse_weight, up_weight=up_weight, fine_weight=fine_weight, coarse_bias=coarse_bias, fine_bias=fine_bias)


def headings():
    face_steps = [(1, 0, 0), (-1, 0, 0), (0, 1, 0), (0, -1, 0), (0, 0, 1), (0, 0, -1)]
    others = []
    for step_x in (-1, 0, 1):
        for step_y in (-1, 0, 1):
            for step_z in (-1, 0, 1):
                if abs(step_x) + abs(step_y) + abs(step_z) >= 2:
                    others.append((step_x, step_y, step_z))
    return face_steps + others


def source_span(edge_cells, heading):
    return [(0, 1) if along == 1 else ((edge_cells - 1, edge_cells) if along == -1 else (0, edge_cells)) for along in heading]


def target_span(edge_cells, heading):
    return [(edge_cells + 1, edge_cells + 2) if along == 1 else ((0, 1) if along == -1 else (1, edge_cells + 1)) for along in heading]


def outer_pieces(blocks):
    edge_cells = blocks.shape[-1]
    face_list = []
    rim_list = []
    for number, heading in enumerate(headings()):
        bounds = source_span(edge_cells, heading)
        section = blocks[:, :, bounds[0][0]:bounds[0][1], bounds[1][0]:bounds[1][1], bounds[2][0]:bounds[2][1]]
        section = section.reshape(blocks.shape[0], blocks.shape[1], -1)
        if number < 6:
            face_list.append(section)
        else:
            rim_list.append(jnp.pad(section, ((0, 0), (0, 0), (0, edge_cells - section.shape[2]))))
    return jnp.stack(face_list, 1), jnp.stack(rim_list, 1)


def framed(centre, face_rows, rim_rows):
    edge_cells = centre.shape[-1]
    padded = jnp.pad(centre, ((0, 0), (0, 0), (1, 1), (1, 1), (1, 1)))
    for number, heading in enumerate(headings()):
        bounds = target_span(edge_cells, heading)
        extent = [limits[1] - limits[0] for limits in bounds]
        volume = extent[0] * extent[1] * extent[2]
        section = face_rows[:, number] if number < 6 else rim_rows[:, number - 6]
        section = section[:, :, :volume].reshape((centre.shape[0], centre.shape[1], extent[0], extent[1], extent[2]))
        padded = padded.at[:, :, bounds[0][0]:bounds[0][1], bounds[1][0]:bounds[1][1], bounds[2][0]:bounds[2][1]].set(section)
    return padded


def level_conv(field_rows, neighbours, weight, biases, group_size):
    brick_total, channels = field_rows.shape[0], field_rows.shape[1]
    blocks = field_rows.reshape(brick_total, channels, EDGE, EDGE, EDGE)
    face_all, rim_all = outer_pieces(blocks)
    kernel = jnp.transpose(weight, (1, 2, 0)).reshape(channels, channels, 3, 3, 3).astype(jnp.float32)

    def one_group(packed):
        centre, links_here = packed
        clipped = jnp.maximum(links_here, 0)
        present = links_here >= 0
        face_rows = face_all[clipped[:, :6], jnp.arange(6, dtype=jnp.int32)[None, :]]
        face_rows = jnp.where(present[:, :6, None, None], face_rows, jnp.zeros_like(face_rows))
        rim_rows = rim_all[clipped[:, 6:], jnp.arange(20, dtype=jnp.int32)[None, :]]
        rim_rows = jnp.where(present[:, 6:, None, None], rim_rows, jnp.zeros_like(rim_rows))
        padded = framed(centre, face_rows, rim_rows).astype(jnp.float32)
        result = lax.conv_general_dilated(padded, kernel, (1, 1, 1), "VALID", dimension_numbers=("NCDHW", "OIDHW", "NCDHW"), precision=lax.Precision.HIGHEST)
        return jnp.maximum(result + biases[None, :, None, None, None], 0.0).astype(jnp.bfloat16)

    grouped = (blocks.reshape(brick_total // group_size, group_size, channels, EDGE, EDGE, EDGE), neighbours.reshape(brick_total // group_size, group_size, 26))
    return lax.map(one_group, grouped).reshape(brick_total, channels, EDGE ** 3)


def reference(features, fine_links, coarse_links, parents, down_weight, coarse_weight, up_weight, fine_weight, coarse_bias, fine_bias):
    half_edge = EDGE // 2
    octant_size = half_edge ** 3
    brick_total, channels = features.shape[0], features.shape[1]
    coarse_total = coarse_links.shape[0]
    down_float = down_weight.astype(jnp.float32)
    up_float = up_weight.astype(jnp.float32)

    def project(block_rows):
        split_rows = block_rows.reshape(BR_DEV, channels, half_edge, 2, half_edge, 2, half_edge, 2)
        split_rows = jnp.transpose(split_rows, (0, 3, 5, 7, 1, 2, 4, 6)).reshape(BR_DEV, 8, channels, octant_size)
        summed = jnp.einsum("oed,bodu->beu", down_float, split_rows.astype(jnp.float32), precision=lax.Precision.HIGHEST)
        return summed.astype(jnp.bfloat16)

    projected = lax.map(project, features.reshape(brick_total // BR_DEV, BR_DEV, channels, EDGE ** 3))
    projected = projected.reshape(brick_total, channels, octant_size)
    summed = jax.ops.segment_sum(projected.astype(jnp.float32), parents, num_segments=8 * coarse_total)
    summed = summed.reshape(coarse_total, 2, 2, 2, channels, half_edge, half_edge, half_edge)
    coarse_in = jnp.transpose(summed, (0, 4, 1, 5, 2, 6, 3, 7)).reshape(coarse_total, channels, EDGE ** 3).astype(jnp.bfloat16)
    coarse_out = level_conv(coarse_in, coarse_links, coarse_weight, coarse_bias, CBR_DEV)
    octant_rows = coarse_out.reshape(coarse_total, channels, 2, half_edge, 2, half_edge, 2, half_edge)
    octant_rows = jnp.transpose(octant_rows, (0, 2, 4, 6, 1, 3, 5, 7)).reshape(8 * coarse_total, channels, octant_size)

    def lift(packed):
        rows_here, codes_here = packed
        octants = octant_rows[codes_here].astype(jnp.float32)
        upsampled = jnp.einsum("oec,bcu->boeu", up_float, octants, precision=lax.Precision.HIGHEST)
        upsampled = upsampled.reshape(BR_DEV, 2, 2, 2, channels, half_edge, half_edge, half_edge)
        upsampled = jnp.transpose(upsampled, (0, 4, 5, 1, 6, 2, 7, 3)).reshape(BR_DEV, channels, EDGE ** 3)
        return (rows_here.astype(jnp.float32) + upsampled).astype(jnp.bfloat16)

    merged = lax.map(lift, (features.reshape(brick_total // BR_DEV, BR_DEV, channels, EDGE ** 3), parents.reshape(brick_total // BR_DEV, BR_DEV)))
    merged = merged.reshape(brick_total, channels, EDGE ** 3)
    return level_conv(merged, fine_links, fine_weight, fine_bias, BR_DEV)
```

```python
import functools

import jax
import jax.numpy as jnp
import numpy as np
from jax import lax
from jax.experimental import pallas as pl
from jax.experimental.pallas import tpu as pltpu
from jax.sharding import PartitionSpec as P

EDGE = 8
NX, NZ, NC = 4, 16, 2
PEERS = NX * NZ * NC
NY = 4
HALO = 144
MESH = pl.DeviceIdType.MESH
BF16 = jnp.bfloat16
F32 = jnp.float32


def headings():
    faces = [(1, 0, 0), (-1, 0, 0), (0, 1, 0), (0, -1, 0), (0, 0, 1), (0, 0, -1)]
    steps = [(a, b, c) for a in (-1, 0, 1) for b in (-1, 0, 1) for c in (-1, 0, 1)]
    return faces + [d for d in steps if sum(map(abs, d)) >= 2]


NUMBER = {d: k for k, d in enumerate(headings())}


def inner_row(fine, cell):
    if fine:
        low = [c // 2 for c in cell]
        part = [c % 2 for c in cell]
    else:
        low = [c % 4 for c in cell]
        part = [c // 4 for c in cell]
    return low[0], (4 * part[0] + 2 * part[1] + part[2]) * 16 + low[1] * 4 + low[2]


def halo_row(d, cell):
    k = NUMBER[d]
    free = [cell[n] for n in range(3) if d[n] == 0]
    if len(free) == 2:
        return free[0] // 2, 16 * k + (free[0] % 2) * 8 + free[1]
    if len(free) == 1:
        return free[0] // 2, 96 + 2 * (k - 6) + free[0] % 2
    return 0, 96 + 2 * (k - 6)


def frame_planes(fine, j):
    return [2 * j + n for n in range(4)] if fine else [j, j + 1, j + 2, j + 4, j + 5, j + 6]


def frame_tables(fine):
    inner, outer = [], []
    for j in range(NY):
        rows_in, rows_out = [], []
        for a3 in range(3):
            for px in frame_planes(fine, j):
                for py in range(10):
                    for z in range(8):
                        at = (px, py, z + a3)
                        d = tuple(1 if v == 9 else -1 if v == 0 else 0 for v in at)
                        cell = tuple(v - 1 for v in at)
                        if d == (0, 0, 0):
                            q, r = inner_row(fine, cell)
                            rows_in.append(q * 128 + r)
                            rows_out.append(-1)
                        else:
                            q, r = halo_row(d, cell)
                            rows_in.append(-1)
                            rows_out.append(q * HALO + r)
        inner.append(rows_in)
        outer.append(rows_out)
    return np.array(inner, np.int32), np.array(outer, np.int32)


def piece_tables(fine):
    table = np.full((NY, HALO), -1, np.int32)
    for d in headings():
        edge = [0 if v == 1 else 7 for v in d]
        spans = [range(8) if v == 0 else (e,) for v, e in zip(d, edge)]
        for x in spans[0]:
            for y in spans[1]:
                for z in spans[2]:
                    cell = (x, y, z)
                    quarter, row = halo_row(d, cell)
                    q, r = inner_row(fine, cell)
                    table[quarter, row] = q * 128 + r
    return table


def unfold_table():
    rows = []
    for o in range(8):
        for u in range(16):
            x, y, z = o // 4, 2 * (u // 4) + (o // 2) % 2, 2 * (u % 4) + o % 2
            rows.append(x * 64 + y * 8 + z)
    return np.array(rows, np.int32)


def octant_table():
    rows = []
    for q in range(4):
        for u in range(16):
            rows.append((4 * (q // 2) + u // 4) * 8 + 4 * (q % 2) + u % 4)
    return np.array(rows, np.int32)


def picks(rows, width):
    return (rows[..., None] == jnp.arange(width, dtype=jnp.int32)).astype(BF16)


def place(owner):
    return owner // (NZ * NC), (owner // NC) % NZ, owner % NC


def shift_of(slot):
    j = slot // 8
    dz = jnp.where(j % 2 == 1, (j + 1) // 2, (NZ - j // 2) % NZ)
    return (slot % 8) // 2, dz, slot % 2


def dest_of(me, slot):
    x, z, c = place(me)
    dx, dz, dc = shift_of(slot)
    return ((x + dx) % NX * NZ + (z + dz) % NZ) * NC + (c + dc) % NC


def slot_from(me, owner):
    x, z, c = place(me)
    ox, oz, oc = place(owner)
    dx, dz, dc = (x - ox) % NX, (z - oz) % NZ, (c - oc) % NC
    j = jnp.where(dz == 0, 0, jnp.where(dz <= NZ // 2, 2 * dz - 1, 2 * (NZ - dz)))
    return j * 8 + dx * 2 + dc


def answer_slot(slot):
    j = slot // 8
    back = jnp.where(j == 0, 0, jnp.where(j == NZ - 1, j, jnp.where(j % 2 == 1, j + 1, j - 1)))
    return back * 8 + (NX - (slot % 8) // 2) % NX * 2 + slot % 2


AT_CHILD, AT_FF, AT_FR, AT_CF, AT_CR, AT_PAR, TABLE = 0, 128, 152, 232, 244, 284, 288

Y_FEAT, Y_DOWN, Y_BIAS, Y_UP, Y_CW, Y_FW, Y_CG, Y_CH, Y_MG, Y_FH, Y_OUT = range(11)
B_IDX, B_UP, B_CF, B_CR, B_DOWN, B_FF, B_FR = range(7)


def nt(a, b):
    return lax.dot_general(a, b, (((1,), (1,)), ((), ())), preferred_element_type=F32)


def nn(a, b):
    return jnp.dot(a, b, preferred_element_type=F32)


def kernel(
    table, feat, idx_send, down_w, up_w, coarse_w, fine_w, bias, unfold, octant,
    coarse_pick, fine_pick, coarse_inner, coarse_outer, fine_inner, fine_outer,
    out,
    idx_recv, idx_smem, feats, down_all, bias_all, up_all, coarse_w_all, fine_w_all,
    own, child, up_send, up_recv, coarse_all, faces, rims, cf_send, cr_send, cf_recv, cr_recv,
    coarse_halo, frame, columns, octants, down_send, down_recv, merged_all, ff_send, fr_send,
    ff_recv, fr_recv, fine_halo, rim_rows, out_send, out_recv,
    y_ss, y_rs, b_ss, b_rs, local_sem,
):
    me, y = lax.axis_index("brick"), lax.axis_index("chan")

    barrier = pltpu.get_barrier_semaphore()

    def greet(s, carry):
        pl.semaphore_signal(barrier, inc=1, device_id={"brick": dest_of(me, s)}, device_id_type=MESH)
        return carry

    lax.fori_loop(1, PEERS, greet, 0)
    for k in range(1, NY):
        pl.semaphore_signal(barrier, inc=1, device_id={"chan": (y + k) % NY}, device_id_type=MESH)
    pl.semaphore_wait(barrier, PEERS - 1 + NY - 1)

    def y_copies(phase, src, dst):
        return [
            pltpu.make_async_remote_copy(
                src_ref=src((y + k) % NY), dst_ref=dst, send_sem=y_ss.at[phase, k - 1],
                recv_sem=y_rs.at[phase, k - 1], device_id={"chan": (y + k) % NY}, device_id_type=MESH,
            )
            for k in range(1, NY)
        ]

    def y_start(copies):
        for c in copies:
            c.start()

    def y_arrived(copies):
        for c in copies:
            c.wait_recv()

    def b_copy(phase, src, dst, s):
        return pltpu.make_async_remote_copy(
            src_ref=src.at[s], dst_ref=dst.at[s], send_sem=b_ss.at[phase], recv_sem=b_rs.at[phase],
            device_id={"brick": dest_of(me, s)}, device_id_type=MESH,
        )

    def b_all(phase, src, dst):
        return pltpu.make_async_remote_copy(
            src_ref=src.at[pl.ds(1, PEERS - 1)], dst_ref=dst.at[pl.ds(1, PEERS - 1)],
            send_sem=b_ss.at[phase], recv_sem=b_rs.at[phase],
            device_id={"brick": dest_of(me, 1)}, device_id_type=MESH,
        )

    def b_start(*exchanges):
        def send(t, carry):
            for phase, src, dst in exchanges:
                b_copy(phase, src, dst, PEERS - 1 - t).start()
            return carry

        lax.fori_loop(0, PEERS - 1, send, 0)

    def mine(ref):
        return ref.at[y]

    feat_copies = y_copies(Y_FEAT, lambda p: feat.at[:, :, pl.ds(pl.multiple_of(p * 128, 128), 128)],
                           feats.at[:, pl.ds(pl.multiple_of(y * 32, 32), 32), :])
    y_start(feat_copies)
    down_copies = y_copies(Y_DOWN, lambda p: down_w, mine(down_all))
    y_start(down_copies)
    b_start((B_IDX, idx_send, idx_recv))
    later = []
    for phase, src, dst in ((Y_BIAS, bias, bias_all), (Y_CW, coarse_w, coarse_w_all),
                            (Y_UP, up_w, up_all), (Y_FW, fine_w, fine_w_all)):
        copies = y_copies(phase, lambda p, src=src: src, mine(dst))
        y_start(copies)
        later.append(copies)
    feats[:, pl.ds(pl.multiple_of(y * 32, 32), 32), :] = (
        feat[:, :, pl.ds(pl.multiple_of(y * 128, 128), 128)])
    down_all[y] = down_w[...]
    bias_all[y] = bias[...]
    coarse_w_all[y] = coarse_w[...]
    up_all[y] = up_w[...]
    fine_w_all[y] = fine_w[...]
    idx_recv[0] = idx_send[0]

    y_arrived(feat_copies)
    y_arrived(down_copies)
    for b in range(4):
        own[b] = nt(unfold[...], feats[b]).astype(BF16)
    total = jnp.zeros((64, 128), F32)
    for o in range(8):
        rows = jnp.concatenate([own[b, 16 * o:16 * o + 16, :] for b in range(4)], axis=0)
        weight = jnp.concatenate([down_all[i, o] for i in range(NY)], axis=0)
        total = total + nn(rows, weight)
    child[...] = total.astype(BF16).reshape(4, 16, 128)

    def give_child(t, carry):
        s = PEERS - 1 - t
        up_send[s] = child[table[AT_CHILD + s]]
        return carry

    lax.fori_loop(0, PEERS, give_child, 0, unroll=4)
    b_start((B_UP, up_send, up_recv))
    up_recv[0] = up_send[0]

    zero = jnp.zeros((16, 128), BF16)
    for ref in (cf_recv, ff_recv):
        ref[PEERS] = zero
    for ref in (cr_recv, fr_recv):
        ref[PEERS] = jnp.zeros((2, 128), BF16)
    rim_rows[...] = jnp.zeros(rim_rows.shape, F32)

    idx_all = b_all(B_IDX, idx_send, idx_recv)
    idx_all.wait_recv()
    to_smem = pltpu.make_async_copy(idx_recv, idx_smem, local_sem)
    to_smem.start()
    to_smem.wait()

    up_done = b_all(B_UP, up_send, up_recv)
    up_done.wait_recv()
    row = lax.broadcasted_iota(jnp.int32, (256, 128), 0)
    lane = lax.broadcasted_iota(jnp.int32, (256, 128), 1)
    same = row % 16 == lane % 16
    wide = lax.broadcasted_iota(jnp.int32, (1, 128), 1) // 16

    def add_children(g, acc):
        codes = jnp.zeros((1, 128), jnp.int32)
        for i in range(8):
            codes = jnp.where(wide == i, idx_smem[8 * g + i, 0, 4], codes)
        hot = jnp.where(same & (row // 16 == codes), 1.0, 0.0).astype(BF16)
        return acc + nn(hot, up_recv[pl.ds(8 * g, 8)].reshape(128, 128))

    summed = lax.fori_loop(0, PEERS // 8, add_children, jnp.zeros((256, 128), F32))
    coarse_all[y] = summed.astype(BF16).reshape(2, 128, 128)
    gather = y_copies(Y_CG, lambda p: mine(coarse_all), mine(coarse_all))
    y_start(gather)
    y_arrived(gather)

    def halo(bricks, whole, pick, f_field, at_f, at_r, f_phase, r_phase, y_phase,
             f_send, r_send, f_recv, r_recv, halo_all, inner, outer, rows):
        for b in range(bricks):
            source = jnp.concatenate([whole[i, b] for i in range(NY)], axis=0)
            found = nn(pick[...], source)
            faces[pl.ds(6 * b, 6)] = found[:96].astype(BF16).reshape(6, 16, 128)
            for r in range(20):
                rims[20 * b + r] = found[96 + 2 * r:98 + 2 * r].astype(BF16)

        def answer(t, carry):
            s = PEERS - 1 - t
            asker = answer_slot(s)
            f_send[s] = faces[idx_smem[asker, 0, f_field]]
            r_send[s] = rims[idx_smem[asker, 0, f_field + 1]]
            return carry

        lax.fori_loop(0, PEERS, answer, 0, unroll=4)
        b_start((f_phase, f_send, f_recv), (r_phase, r_send, r_recv))
        f_recv[0] = f_send[0]
        r_recv[0] = r_send[0]
        for b in range(bricks):
            source = jnp.concatenate([whole[i, b] for i in range(NY)], axis=0)
            frame[b, 0:rows, :] = nn(inner[...], source)
        waits = [b_all(f_phase, f_send, f_recv), b_all(r_phase, r_send, r_recv)]
        for w in waits:
            w.wait_recv()
        for b in range(bricks):
            for k in range(6):
                halo_all[y, b, 16 * k:16 * k + 16, :] = f_recv[table[at_f + 6 * b + k]]
            for r in range(20):
                rim_rows[b, 2 * r:2 * r + 2, :] = r_recv[table[at_r + 20 * b + r]].astype(F32)
            halo_all[y, b, 96:144, :] = rim_rows[b].astype(BF16)
        around = y_copies(y_phase, lambda p: mine(halo_all), mine(halo_all))
        y_start(around)
        y_arrived(around)
        for b in range(bricks):
            source = jnp.concatenate([halo_all[i, b] for i in range(NY)], axis=0)
            frame[b, 0:rows, :] = frame[b, 0:rows, :] + nn(outer[...], source)
        return waits, around

    def conv(bricks, planes, starts, weights, bias_row):
        for tap in range(27):
            a, a2, a3 = tap // 9, (tap // 3) % 3, tap % 3
            for b in range(bricks):
                for n, start in enumerate(starts):
                    at = ((a3 * planes + start + a) * 10 + a2) * 8
                    columns[(2 * b + n) * 64:(2 * b + n + 1) * 64, tap * 128:tap * 128 + 128] = (
                        frame[b, at:at + 64, :].astype(BF16))
        weight = jnp.concatenate([weights[i] for i in range(NY)], axis=0)
        whole = nt(columns[0:bricks * 128, :], weight)
        shift = bias_all[0] + bias_all[1] + bias_all[2] + bias_all[3]
        return jnp.maximum(whole + shift[bias_row:bias_row + 1, :], 0.0)

    coarse_waits, coarse_around = halo(
        2, coarse_all, coarse_pick, 2, AT_CF, AT_CR, B_CF, B_CR, Y_CH,
        cf_send, cr_send, cf_recv, cr_recv, coarse_halo, coarse_inner, coarse_outer, 1440)
    for copies in later:
        y_arrived(copies)
    coarse_out = conv(2, 6, (0, 3), coarse_w_all, 0).astype(BF16)
    for p in range(2):
        for n in range(2):
            at = (2 * p + n) * 64
            octants[pl.ds(8 * p + 4 * n, 4)] = (
                nn(octant[...], coarse_out[at:at + 64]).astype(BF16).reshape(4, 16, 128))

    def give_octant(t, carry):
        s = PEERS - 1 - t
        down_send[s] = octants[jnp.maximum(idx_smem[answer_slot(s), 0, 4], 0)]
        return carry

    lax.fori_loop(0, PEERS, give_octant, 0, unroll=4)
    b_start((B_DOWN, down_send, down_recv))
    down_recv[0] = down_send[0]
    down_done = b_all(B_DOWN, down_send, down_recv)
    down_done.wait_recv()
    coarse_rows = jnp.concatenate([down_recv[table[AT_PAR + b]] for b in range(4)], axis=0)
    for o in range(8):
        weight = jnp.concatenate([up_all[i, o] for i in range(NY)], axis=0)
        lifted = nt(coarse_rows, weight)
        for b in range(4):
            merged_all[y, b, 16 * o:16 * o + 16, :] = (
                own[b, 16 * o:16 * o + 16, :].astype(F32) + lifted[16 * b:16 * b + 16]).astype(BF16)
    merge = y_copies(Y_MG, lambda p: mine(merged_all), mine(merged_all))
    y_start(merge)
    y_arrived(merge)

    fine_waits, fine_around = halo(
        4, merged_all, fine_pick, 0, AT_FF, AT_FR, B_FF, B_FR, Y_FH,
        ff_send, fr_send, ff_recv, fr_recv, fine_halo, fine_inner, fine_outer, 960)
    refined = conv(4, 4, (0, 1), fine_w_all, 1)
    for b in range(4):
        out_send[b] = refined[128 * b:128 * b + 128].T.astype(BF16)
    back = y_copies(Y_OUT, lambda p: out_send.at[:, pl.ds(pl.multiple_of(p * 32, 32), 32), :],
                    mine(out_recv))
    y_start(back)
    out_recv[y] = out_send[:, pl.ds(pl.multiple_of(y * 32, 32), 32), :]
    y_arrived(back)
    for i in range(NY):
        out[:, :, 128 * i:128 * i + 128] = out_recv[i]

    for w in [idx_all, up_done, down_done] + coarse_waits + fine_waits:
        w.wait_send()
    for copies in [feat_copies, down_copies, gather, coarse_around, merge, fine_around, back] + later:
        for c in copies:
            c.wait_send()


def requests(links, per_owner, dest):
    listed = links.reshape(1, -1)
    number = jnp.arange(links.shape[1], dtype=jnp.int32)[None, :]
    wanted = (links % per_owner * links.shape[1] + number).reshape(1, -1)
    hit = (listed >= 0) & (listed // per_owner == dest[:, None])
    return jnp.sum(jnp.where(hit, wanted, 0), axis=1)


def per_device(features, fine_links, coarse_links, parents, down_weight, coarse_weight, up_weight,
               fine_weight, coarse_bias, fine_bias):
    me, y = lax.axis_index("brick"), lax.axis_index("chan")
    dest = dest_of(me, jnp.arange(PEERS, dtype=jnp.int32))
    home = parents // 16
    there = home[None, :] == dest[:, None]
    code = jnp.sum(jnp.where(there, parents[None, :] % 16 + 1, 0), axis=1) - 1
    child = jnp.sum(jnp.where(there, jnp.arange(4, dtype=jnp.int32)[None, :], 0), axis=1)
    ask = jnp.stack([
        requests(fine_links[:, :6], 4, dest), requests(fine_links[:, 6:], 4, dest),
        requests(coarse_links[:, :6], 2, dest), requests(coarse_links[:, 6:], 2, dest), code], axis=1)
    idx_send = jnp.pad(ask, ((0, 0), (0, 123)))[:, None, :]

    def found(links, per_owner):
        flat = links.reshape(-1)
        return jnp.where(flat >= 0, slot_from(me, flat // per_owner), PEERS)

    table = jnp.concatenate([
        child, found(fine_links[:, :6], 4), found(fine_links[:, 6:], 4),
        found(coarse_links[:, :6], 2), found(coarse_links[:, 6:], 2), slot_from(me, home)])
    ci, co = frame_tables(False)
    fi, fo = frame_tables(True)
    mine = lambda t: lax.dynamic_index_in_dim(jnp.asarray(t), y, 0, keepdims=False)
    bias = jnp.stack([coarse_bias, fine_bias])
    bias = lax.dynamic_update_slice(jnp.zeros((8, 128), F32), bias, (0, y * 32))
    args = (
        table, features, idx_send,
        jnp.transpose(down_weight, (0, 2, 1)), up_weight,
        jnp.transpose(coarse_weight, (1, 0, 2)).reshape(32, 27 * 128),
        jnp.transpose(fine_weight, (1, 0, 2)).reshape(32, 27 * 128), bias,
        picks(jnp.asarray(unfold_table()), 128), picks(jnp.asarray(octant_table()), 64),
        picks(mine(piece_tables(False)), 512), picks(mine(piece_tables(True)), 512),
        picks(mine(ci), 512), picks(mine(co), 4 * HALO), picks(mine(fi), 512), picks(mine(fo), 4 * HALO),
    )
    v = pltpu.VMEM
    scratch = dict(
        idx_recv=v((128, 1, 128), jnp.int32), idx_smem=pltpu.SMEM((128, 1, 128), jnp.int32),
        feats=v((4, 128, 128), BF16), down_all=v((4, 8, 32, 128), BF16), bias_all=v((4, 8, 128), F32),
        up_all=v((4, 8, 32, 128), BF16), coarse_w_all=v((4, 32, 3456), BF16),
        fine_w_all=v((4, 32, 3456), BF16), own=v((4, 128, 128), BF16), child=v((4, 16, 128), BF16),
        up_send=v((128, 16, 128), BF16), up_recv=v((128, 16, 128), BF16),
        coarse_all=v((4, 2, 128, 128), BF16), faces=v((24, 16, 128), BF16), rims=v((80, 2, 128), BF16),
        cf_send=v((128, 16, 128), BF16), cr_send=v((128, 2, 128), BF16),
        cf_recv=v((129, 16, 128), BF16), cr_recv=v((129, 2, 128), BF16),
        coarse_halo=v((4, 2, HALO, 128), BF16), frame=v((4, 1440, 128), F32),
        columns=v((512, 3456), BF16), octants=v((16, 16, 128), BF16),
        down_send=v((128, 16, 128), BF16), down_recv=v((128, 16, 128), BF16),
        merged_all=v((4, 4, 128, 128), BF16),
        ff_send=v((128, 16, 128), BF16), fr_send=v((128, 2, 128), BF16),
        ff_recv=v((129, 16, 128), BF16), fr_recv=v((129, 2, 128), BF16),
        fine_halo=v((4, 4, HALO, 128), BF16), rim_rows=v((4, 48, 128), F32),
        out_send=v((4, 128, 128), BF16), out_recv=v((4, 4, 32, 128), BF16),
        y_ss=pltpu.SemaphoreType.DMA((11, 3)), y_rs=pltpu.SemaphoreType.DMA((11, 3)),
        b_ss=pltpu.SemaphoreType.DMA((7,)), b_rs=pltpu.SemaphoreType.DMA((7,)),
        local_sem=pltpu.SemaphoreType.DMA,
    )
    return pl.pallas_call(
        kernel,
        out_shape=jax.ShapeDtypeStruct((4, 32, 512), BF16),
        in_specs=[pl.BlockSpec(memory_space=pltpu.SMEM)] + [pl.BlockSpec(memory_space=v)] * 15,
        out_specs=pl.BlockSpec(memory_space=v),
        scratch_shapes=list(scratch.values()),
        compiler_params=pltpu.CompilerParams(collective_id=0, has_side_effects=True),
    )(*args)


def solution(mesh):
    in_specs = (
        P("brick", "chan", None), P("brick", None), P("brick", None), P("brick"),
        P(None, None, "chan"), P(None, "chan", None), P(None, "chan", None), P(None, "chan", None),
        P("chan"), P("chan"),
    )
    return jax.shard_map(
        per_device, mesh=mesh, in_specs=in_specs, out_specs=P("brick", "chan", None), check_vma=False
    )
```

```python
import functools

import jax
import jax.numpy as jnp
import numpy as np
from jax import lax
from jax.experimental import pallas as pl
from jax.experimental.pallas import tpu as pltpu
from jax.sharding import PartitionSpec as P

EDGE = 8
NX, NZ, NC = 4, 16, 2
PEERS = NX * NZ * NC
NY = 4
HALO = 144
MESH = pl.DeviceIdType.MESH
BF16 = jnp.bfloat16
F32 = jnp.float32


def headings():
    faces = [(1, 0, 0), (-1, 0, 0), (0, 1, 0), (0, -1, 0), (0, 0, 1), (0, 0, -1)]
    steps = [(a, b, c) for a in (-1, 0, 1) for b in (-1, 0, 1) for c in (-1, 0, 1)]
    return faces + [d for d in steps if sum(map(abs, d)) >= 2]


NUMBER = {d: k for k, d in enumerate(headings())}


def inner_row(fine, cell):
    if fine:
        low = [c // 2 for c in cell]
        part = [c % 2 for c in cell]
    else:
        low = [c % 4 for c in cell]
        part = [c // 4 for c in cell]
    return low[0], (4 * part[0] + 2 * part[1] + part[2]) * 16 + low[1] * 4 + low[2]


def halo_row(fine, d, cell):
    k = NUMBER[d]
    free = [cell[n] for n in range(3) if d[n] == 0]
    if not free:
        return 0, 96 + 2 * (k - 6)
    if d[0] == 0 and not fine:
        quarter, half = free[0] % 4, free[0] // 4
    else:
        quarter, half = free[0] // 2, free[0] % 2
    if len(free) == 2:
        return quarter, 16 * k + half * 8 + free[1]
    return quarter, 96 + 2 * (k - 6) + half


def frame_planes(fine, j):
    return [2 * j + n for n in range(4)] if fine else [j, j + 1, j + 2, j + 4, j + 5, j + 6]


def frame_tables(fine):
    inner, outer = [], []
    for j in range(NY):
        rows_in, rows_out = [], []
        for a3 in range(3):
            for px in frame_planes(fine, j):
                for py in range(10):
                    for z in range(8):
                        at = (px, py, z + a3)
                        d = tuple(1 if v == 9 else -1 if v == 0 else 0 for v in at)
                        cell = tuple(v - 1 for v in at)
                        if d == (0, 0, 0):
                            q, r = inner_row(fine, cell)
                            rows_in.append(q * 128 + r)
                            rows_out.append(-1)
                        else:
                            q, r = halo_row(fine, d, cell)
                            rows_in.append(-1)
                            rows_out.append(q * HALO + r)
        inner.append(rows_in)
        outer.append(rows_out)
    return np.array(inner, np.int32), np.array(outer, np.int32)


def piece_tables(fine):
    table = np.full((NY, HALO), -1, np.int32)
    for d in headings():
        edge = [0 if v == 1 else 7 for v in d]
        spans = [range(8) if v == 0 else (e,) for v, e in zip(d, edge)]
        for x in spans[0]:
            for y in spans[1]:
                for z in spans[2]:
                    cell = (x, y, z)
                    quarter, row = halo_row(fine, d, cell)
                    q, r = inner_row(fine, cell)
                    if x == 0:
                        table[quarter, row] = r
                    elif x == 7:
                        table[quarter, row] = r
                    else:
                        assert q == quarter
                        table[quarter, row] = 128 + r
    return table


def unfold_table():
    rows = []
    for o in range(8):
        for u in range(16):
            x, y, z = o // 4, 2 * (u // 4) + (o // 2) % 2, 2 * (u % 4) + o % 2
            rows.append(x * 64 + y * 8 + z)
    return np.array(rows, np.int32)


def octant_table():
    rows = []
    for q in range(4):
        for u in range(16):
            rows.append((4 * (q // 2) + u // 4) * 8 + 4 * (q % 2) + u % 4)
    return np.array(rows, np.int32)


def row_tables():
    unfold = np.broadcast_to(unfold_table(), (NY, 128))
    octant = np.broadcast_to(octant_table(), (NY, 64))
    frames = []
    for fine in (False, True):
        inner, outer = frame_tables(fine)
        frames.append(np.where(inner >= 0, inner, 512 + outer))
    return np.concatenate(
        [unfold, octant, piece_tables(False), piece_tables(True), frames[0], frames[1]], axis=1)


ROW_UNFOLD, ROW_OCTANT, ROW_CP, ROW_FP, ROW_CF, ROW_FF, ROWS = 0, 128, 192, 336, 480, 1920, 2880


AT_PAR = 52

Y_FEAT, Y_DOWN, Y_BIAS, Y_UP, Y_CW, Y_FW, Y_CG, Y_CG2, Y_CH, Y_MG, Y_MG2, Y_FH, Y_OUT = range(13)
B_IDX, B_IDR, B_UP, B_CF, B_CR, B_DOWN, B_FF, B_FR = range(8)


def nt(a, b):
    return lax.dot_general(a, b, (((1,), (1,)), ((), ())), preferred_element_type=F32)


def nn(a, b):
    return jnp.dot(a, b, preferred_element_type=F32)


def within(index, count):
    return jnp.minimum(jnp.maximum(index, 0), count - 1)


def choose(values, index):
    picked = values[0]
    for n in range(1, len(values)):
        picked = jnp.where(index == n, values[n], picked)
    return picked


def kernel(
    links, feat, link_rows, down_w, up_w, coarse_w, fine_w, bias, row_of,
    out,
    notes, table, asks, idx_smem, unfold, octant, coarse_pick, fine_pick, coarse_inner, coarse_outer,
    fine_inner, fine_outer, coarse_w_flat, fine_w_flat,
    il_recv, ir_recv, feats, down_all, bias_all, up_all, coarse_w_all, fine_w_all,
    own, child, column, relay_send, up_recv, coarse_all, faces, rims, cf_send, cr_send, cf_recv, cr_recv,
    coarse_halo, frame, columns, octants, down_send, down_mid, down_out, down_recv, merged_all, ff_send, fr_send,
    ff_recv, fr_recv, fine_halo, rim_rows, out_send, out_recv,
    y_ss, y_rs, b_ss, b_rs, a_ss, a_rs, d_ss, d_rs, local_sem,
):
    me, y = lax.axis_index("brick"), lax.axis_index("chan")
    x, z, core = me // (NZ * NC), me // NC % NZ, me % NC

    near = [(x + n // 2) % NX * (NZ * NC) + (core + n % 2) % NC for n in range(8)]

    def z_base(j):
        step = (j + 1) // 2
        ahead = z + step
        back = z + NZ - j // 2
        at = (j % 2) * ahead + (1 - j % 2) * back
        return at % NZ * NC

    def pick(dst, first, base, width):
        for at in range(0, width, 128):
            w = min(128, width - at)
            lanes = lax.broadcasted_iota(jnp.int32, (dst.shape[0], w), 1) + (base + at)
            hit = row_of[first:first + dst.shape[0], 0:w] == lanes
            dst[:, at:at + w] = jnp.where(hit, 1.0, 0.0).astype(BF16)

    barrier = pltpu.get_barrier_semaphore()

    def greet(j, base, first):
        for n in range(first, 8):
            pl.semaphore_signal(barrier, inc=1, device_id={"brick": near[n] + base}, device_id_type=MESH)

    def greet_far(t, carry):
        greet(15 - t, z_base(15 - t), 0)
        return carry

    lax.fori_loop(0, 15, greet_far, 0)
    greet(0, z * NC, 1)
    for k in range(1, NY):
        pl.semaphore_signal(barrier, inc=1, device_id={"chan": (y + k) % NY}, device_id_type=MESH)

    def slots(l, owner):
        dx, dz, dc = (x - (owner >> 5)) & 3, (z - (owner >> 1)) & 15, (core - owner) & 1
        j = jnp.where(dz == 0, 0, jnp.where(dz <= 8, 2 * dz - 1, 32 - 2 * dz))
        return j, jnp.where(l >= 0, j * 8 + dx * 2 + dc, PEERS)

    lane = lax.broadcasted_iota(jnp.int32, (1, 128), 1)
    fine_row, coarse_row = link_rows[0], link_rows[1]
    _, notes[0] = slots(fine_row, fine_row >> 2)
    j, slot = slots(coarse_row, jnp.where(lane < AT_PAR, coarse_row >> 1, coarse_row >> 4))
    notes[1] = jnp.where(lane < AT_PAR, slot, j)
    to_table = pltpu.make_async_copy(notes, table, local_sem)
    to_table.start()
    to_table.wait()
    pick(unfold, ROW_UNFOLD, 0, 128)
    pl.semaphore_wait(barrier, PEERS - 1 + NY - 1)

    def y_copies(phase, src, dst):
        return [
            pltpu.make_async_remote_copy(
                src_ref=src((y + k) % NY), dst_ref=dst, send_sem=y_ss.at[phase, k - 1],
                recv_sem=y_rs.at[phase, k - 1], device_id={"chan": (y + k) % NY}, device_id_type=MESH,
            )
            for k in range(1, NY)
        ]

    def y_start(copies):
        for c in copies:
            c.start()

    def y_arrived(copies):
        for c in copies:
            c.wait_recv()

    def b_all(phase, src, dst):
        return pltpu.make_async_remote_copy(
            src_ref=src.at[pl.ds(1, PEERS - 1)], dst_ref=dst.at[pl.ds(1, PEERS - 1)],
            send_sem=b_ss.at[phase], recv_sem=b_rs.at[phase],
            device_id={"brick": near[1] + z * NC}, device_id_type=MESH,
        )

    def send_group(exchanges, j, base, first):
        for n in range(first, 8):
            for phase, src, dst in exchanges:
                pltpu.make_async_remote_copy(
                    src_ref=src(8 * j + n), dst_ref=dst.at[8 * j + n], send_sem=b_ss.at[phase],
                    recv_sem=b_rs.at[phase], device_id={"brick": near[n] + base}, device_id_type=MESH,
                ).start()

    def exchange(exchanges, fill=None):
        def group(t, carry):
            if fill is not None:
                fill(14 - t, 14 - t + (t % 2) * 2 - 1 + jnp.where(t == 14, 1, 0))
            send_group(exchanges, 15 - t, z_base(15 - t), 0)
            return carry

        if fill is not None:
            fill(15, 15)
        lax.fori_loop(0, 15, group, 0)
        send_group(exchanges, 0, z * NC, 1)

    def mine(ref):
        return ref.at[y]

    feat_copies = y_copies(Y_FEAT, lambda p: feat.at[:, :, pl.ds(pl.multiple_of(p * 128, 128), 128)],
                           feats.at[:, pl.ds(pl.multiple_of(y * 32, 32), 32), :])
    y_start(feat_copies)
    down_copies = y_copies(Y_DOWN, lambda p: down_w, mine(down_all))
    y_start(down_copies)
    exchange(((B_IDX, lambda s: link_rows.at[0], il_recv), (B_IDR, lambda s: link_rows.at[1], ir_recv)))
    later = []

    def gather_weights(*weights):
        for phase, src, dst in weights:
            copies = y_copies(phase, lambda p, src=src: src, mine(dst))
            y_start(copies)
            later.append(copies)

    gather_weights((Y_BIAS, bias, bias_all), (Y_CW, coarse_w, coarse_w_all))
    feats[:, pl.ds(pl.multiple_of(y * 32, 32), 32), :] = (
        feat[:, :, pl.ds(pl.multiple_of(y * 128, 128), 128)])
    down_all[y] = down_w[...]
    bias_all[y] = bias[...]
    coarse_w_all[y] = coarse_w[...]
    up_all[y] = up_w[...]
    fine_w_all[y] = fine_w[...]
    il_recv[0] = link_rows[0]
    ir_recv[0] = link_rows[1]

    y_arrived(feat_copies)
    y_arrived(down_copies)
    for b in range(4):
        own[b] = nt(unfold[...], feats[b]).astype(BF16)
    total = jnp.zeros((64, 128), F32)
    for o in range(8):
        rows = jnp.concatenate([own[b, 16 * o:16 * o + 16, :] for b in range(4)], axis=0)
        weight = jnp.concatenate([down_all[i, o] for i in range(NY)], axis=0)
        total = total + nn(rows, weight)
    child[...] = total.astype(BF16).reshape(4, 16, 128)

    def column_copy(j):
        return pltpu.make_async_remote_copy(
            src_ref=child, dst_ref=column.at[j], send_sem=a_ss.at[j], recv_sem=a_rs.at[j],
            device_id={"brick": near[0] + z_base(j)}, device_id_type=MESH,
        )

    for j in range(1, NZ):
        column_copy(j).start()
    column[0] = child[...]

    zero = jnp.zeros((16, 128), BF16)
    for ref in (cf_recv, ff_recv):
        ref[PEERS] = zero
    for ref in (cr_recv, fr_recv):
        ref[PEERS] = jnp.zeros((2, 128), BF16)
    rim_rows[...] = jnp.zeros(rim_rows.shape, F32)

    pick(octant, ROW_OCTANT, 0, 64)
    pick(coarse_pick, ROW_CP, 0, 256)
    pick(coarse_inner, ROW_CF, 0, 512)
    pick(coarse_outer, ROW_CF, 512, 4 * HALO)

    idx_waits = [b_all(B_IDX, il_recv, il_recv), b_all(B_IDR, ir_recv, ir_recv)]
    for w in idx_waits:
        w.wait_recv()

    at = lax.broadcasted_iota(jnp.int32, (1, 1, 128), 2)

    k = at
    for n in (104, 78, 52, 26):
        k = jnp.where(at >= n, jnp.minimum(k, at - n), k)
    face, coarse, parent = k < 6, at < AT_PAR, (at >= AT_PAR) & (at < AT_PAR + 4)
    seen = il_recv[...]
    place_in = jnp.where(face, (seen & 3) * 6 + k, (seen & 3) * 20 + (k - 6))
    fine_ask = jnp.where((seen >> 2 == me) & (at < 104), place_in, 0)
    seen = ir_recv[...]
    place_in = jnp.where(face, (seen & 1) * 6 + k, (seen & 1) * 20 + (k - 6))
    coarse_ask = jnp.where((seen >> 1 == me) & coarse, place_in, 0)
    code_ask = jnp.where((seen >> 4 == me) & parent, (seen & 15) + 1, 0)
    total_asks = jnp.zeros((PEERS, 1, 128), jnp.int32)
    for field, v in enumerate((
            jnp.where(face, fine_ask, 0), jnp.where(face, 0, fine_ask),
            jnp.where(face, coarse_ask, 0), jnp.where(face, 0, coarse_ask), code_ask)):
        got = jnp.max(v, axis=2, keepdims=True)
        total_asks = jnp.where(at == field, got - (1 if field == 4 else 0), total_asks)
    asks[0:PEERS] = total_asks
    seen = jnp.concatenate([ir_recv[8 * j:8 * j + 1] for j in range(NZ)], axis=0)
    sent = jnp.zeros((NZ, 1, 128), jnp.int32)
    for n in range(8):
        v = jnp.where((seen >> 4 == near[n] + z * NC) & parent, at - AT_PAR, 0)
        got = jnp.max(v, axis=2, keepdims=True)
        sent = jnp.where(at == n, got, sent)
    asks[PEERS:PEERS + NZ] = jnp.where(
        parent, ((x - (seen >> 9)) & 3) * 2 + ((core - (seen >> 4)) & 1), sent)
    to_smem = pltpu.make_async_copy(asks, idx_smem, local_sem)
    to_smem.start()
    to_smem.wait()

    def relay_copy(n, g):
        return pltpu.make_async_remote_copy(
            src_ref=relay_send.at[n, pl.ds(4 * g, 4)], dst_ref=up_recv.at[n, pl.ds(4 * g, 4)],
            send_sem=b_ss.at[B_UP], recv_sem=b_rs.at[B_UP],
            device_id={"brick": near[n] + z * NC}, device_id_type=MESH,
        )

    for g in range(NZ // 4):
        for j in range(4 * g, 4 * g + 4):
            if j:
                column_copy(j).wait_recv()
        for j in range(4 * g, 4 * g + 4):
            children = [column[j, b] for b in range(4)]
            up_recv[0, j] = choose(children, idx_smem[PEERS + j, 0, 0])
            for n in range(1, 8):
                relay_send[n, j] = choose(children, idx_smem[PEERS + j, 0, n])
        for n in range(1, 8):
            relay_copy(n, g).start()

    up_done = pltpu.make_async_remote_copy(
        src_ref=relay_send.at[pl.ds(1, 7)], dst_ref=up_recv.at[pl.ds(1, 7)],
        send_sem=b_ss.at[B_UP], recv_sem=b_rs.at[B_UP],
        device_id={"brick": near[1] + z * NC}, device_id_type=MESH,
    )
    up_done.wait_recv()
    row = lax.broadcasted_iota(jnp.int32, (256, 128), 0)
    lane = lax.broadcasted_iota(jnp.int32, (256, 128), 1)
    same = row % 16 == lane % 16
    wide = lax.broadcasted_iota(jnp.int32, (1, 128), 1) // 16

    def add_children(g, acc):
        codes = jnp.zeros((1, 128), jnp.int32)
        for i in range(8):
            codes = jnp.where(wide == i, idx_smem[8 * (g % 2 * 8 + i) + g // 2, 0, 4], codes)
        hot = jnp.where(same & (row // 16 == codes), 1.0, 0.0).astype(BF16)
        return acc + nn(hot, up_recv[g // 2, pl.ds(g % 2 * 8, 8)].reshape(128, 128))

    summed = lax.fori_loop(0, PEERS // 8, add_children, jnp.zeros((256, 128), F32))
    coarse_all[y] = summed.astype(BF16).reshape(2, 128, 128)

    def in_halves(ref, first, second):
        copies = []
        for phase, half in ((first, y // 3), (second, 1 - y // 3)):
            part = ref.at[y, :, pl.ds(pl.multiple_of(64 * half, 64), 64), :]
            copies.append(y_copies(phase, lambda p, part=part: part, part))
            y_start(copies[-1])
        y_arrived(copies[0])
        return copies

    gather = in_halves(coarse_all, Y_CG, Y_CG2)
    gather_weights((Y_UP, up_w, up_all), (Y_FW, fine_w, fine_w_all))

    def halo(bricks, whole, pieces, f_field, link_row, f_phase, r_phase, y_phase,
             f_send, r_send, f_recv, r_recv, halo_all, inner, outer, rows, halves, meanwhile):
        for b in range(bricks):
            source = jnp.concatenate(
                [whole[0, b, 0:64, :], whole[NY - 1, b, 64:128, :], whole[y, b]], axis=0)
            found = nn(pieces[...], source)
            faces[pl.ds(6 * b, 6)] = found[:96].astype(BF16).reshape(6, 16, 128)
            for r in range(20):
                rims[20 * b + r] = found[96 + 2 * r:98 + 2 * r].astype(BF16)

        def answer(j, back):
            for n in range(8):
                asker = 8 * back + (NX - n // 2) % NX * 2 + n % 2
                f_send[8 * j + n] = faces[within(idx_smem[asker, 0, f_field], 6 * bricks)]
                r_send[8 * j + n] = rims[within(idx_smem[asker, 0, f_field + 1], 20 * bricks)]

        exchange(((f_phase, lambda s: f_send.at[s], f_recv), (r_phase, lambda s: r_send.at[s], r_recv)),
                 answer)
        f_recv[0] = f_send[0]
        r_recv[0] = r_send[0]
        meanwhile()
        y_arrived(halves[1])
        for b in range(bricks):
            source = jnp.concatenate([whole[i, b] for i in range(NY)], axis=0)
            frame[b, 0:rows, :] = nn(inner[...], source)
        waits = [b_all(f_phase, f_send, f_recv), b_all(r_phase, r_send, r_recv)]
        for w in waits:
            w.wait_recv()
        for b in range(bricks):
            for k in range(6):
                halo_all[y, b, 16 * k:16 * k + 16, :] = f_recv[within(table[link_row, 0, 26 * b + k], PEERS + 1)]
            for r in range(20):
                rim_rows[b, 2 * r:2 * r + 2, :] = r_recv[within(table[link_row, 0, 26 * b + 6 + r], PEERS + 1)].astype(F32)
            halo_all[y, b, 96:144, :] = rim_rows[b].astype(BF16)
        around = y_copies(y_phase, lambda p: mine(halo_all), mine(halo_all))
        y_start(around)
        y_arrived(around)
        for b in range(bricks):
            source = jnp.concatenate([halo_all[i, b] for i in range(NY)], axis=0)
            frame[b, 0:rows, :] = frame[b, 0:rows, :] + nn(outer[...], source)
        return waits, around

    def conv(bricks, planes, starts, weights, bias_row):
        for tap in range(27):
            a, a2, a3 = tap // 9, (tap // 3) % 3, tap % 3
            for b in range(bricks):
                for n, start in enumerate(starts):
                    at = ((a3 * planes + start + a) * 10 + a2) * 8
                    columns[(2 * b + n) * 64:(2 * b + n + 1) * 64, tap * 128:tap * 128 + 128] = (
                        frame[b, at:at + 64, :].astype(BF16))
        whole = nt(columns[0:bricks * 128, :], weights[...])
        shift = bias_all[0] + bias_all[1] + bias_all[2] + bias_all[3]
        return jnp.maximum(whole + shift[bias_row:bias_row + 1, :], 0.0)

    def flatten_weights():
        for copies in later:
            y_arrived(copies)
        for tap in range(27):
            for i in range(NY):
                for src, dst in ((coarse_w_all, coarse_w_flat), (fine_w_all, fine_w_flat)):
                    dst[32 * i:32 * i + 32, tap * 128:tap * 128 + 128] = src[i, tap]
        pick(fine_pick, ROW_FP, 0, 256)
        pick(fine_inner, ROW_FF, 0, 512)
        pick(fine_outer, ROW_FF, 512, 4 * HALO)

    coarse_waits, coarse_around = halo(
        2, coarse_all, coarse_pick, 2, 1, B_CF, B_CR, Y_CH,
        cf_send, cr_send, cf_recv, cr_recv, coarse_halo, coarse_inner, coarse_outer, 1440,
        gather, flatten_weights)
    coarse_out = conv(2, 6, (0, 3), coarse_w_flat, 0).astype(BF16)
    for p in range(2):
        for n in range(2):
            at = (2 * p + n) * 64
            octants[pl.ds(8 * p + 4 * n, 4)] = (
                nn(octant[...], coarse_out[at:at + 64]).astype(BF16).reshape(4, 16, 128))

    def plane_copy(n, g):
        return pltpu.make_async_remote_copy(
            src_ref=down_send.at[n, pl.ds(4 * g, 4)], dst_ref=down_mid.at[n, pl.ds(4 * g, 4)],
            send_sem=d_ss.at[g], recv_sem=d_rs.at[g],
            device_id={"brick": near[n] + z * NC}, device_id_type=MESH,
        )

    def plane_all(g):
        return pltpu.make_async_remote_copy(
            src_ref=down_send.at[pl.ds(1, 7), pl.ds(4 * g, 4)],
            dst_ref=down_mid.at[pl.ds(1, 7), pl.ds(4 * g, 4)],
            send_sem=d_ss.at[g], recv_sem=d_rs.at[g],
            device_id={"brick": near[1] + z * NC}, device_id_type=MESH,
        )

    def back_of(j):
        return j if j in (0, NZ - 1) else j + 1 if j % 2 else j - 1

    for g in range(NZ // 4 - 1, -1, -1):
        for j in range(4 * g, 4 * g + 4):
            for n in range(8):
                asker = 8 * back_of(j) + (NX - n // 2) % NX * 2 + n % 2
                found = octants[within(idx_smem[asker, 0, 4], 16)]
                if n:
                    down_send[n, j] = found
                else:
                    down_mid[0, j] = found
        for n in range(1, 8):
            plane_copy(n, g).start()
    for g in range(NZ // 4 - 1, -1, -1):
        plane_all(g).wait_recv()
        for j in range(4 * g, 4 * g + 4):
            arrived = [down_mid[n, j] for n in range(8)]
            for b in range(4):
                down_out[j, b] = choose(arrived, idx_smem[PEERS + back_of(j), 0, AT_PAR + b])
        for j in range(4 * g + 3, 4 * g - 1, -1):
            if j:
                pltpu.make_async_remote_copy(
                    src_ref=down_out.at[j], dst_ref=down_recv.at[j], send_sem=b_ss.at[B_DOWN],
                    recv_sem=b_rs.at[B_DOWN], device_id={"brick": near[0] + z_base(j)},
                    device_id_type=MESH,
                ).start()
    down_recv[0] = down_out[0]
    down_done = pltpu.make_async_remote_copy(
        src_ref=down_out.at[pl.ds(1, NZ - 1)], dst_ref=down_recv.at[pl.ds(1, NZ - 1)],
        send_sem=b_ss.at[B_DOWN], recv_sem=b_rs.at[B_DOWN],
        device_id={"brick": near[0] + z_base(1)}, device_id_type=MESH,
    )
    down_done.wait_recv()
    coarse_rows = jnp.concatenate([down_recv[within(table[1, 0, AT_PAR + b], NZ), b] for b in range(4)], axis=0)
    for o in range(8):
        weight = jnp.concatenate([up_all[i, o] for i in range(NY)], axis=0)
        lifted = nt(coarse_rows, weight)
        for b in range(4):
            merged_all[y, b, 16 * o:16 * o + 16, :] = (
                own[b, 16 * o:16 * o + 16, :].astype(F32) + lifted[16 * b:16 * b + 16]).astype(BF16)
    merge = in_halves(merged_all, Y_MG, Y_MG2)

    fine_waits, fine_around = halo(
        4, merged_all, fine_pick, 0, 0, B_FF, B_FR, Y_FH,
        ff_send, fr_send, ff_recv, fr_recv, fine_halo, fine_inner, fine_outer, 960,
        merge, lambda: None)
    refined = conv(4, 4, (0, 1), fine_w_flat, 1)
    for b in range(4):
        out_send[b] = refined[128 * b:128 * b + 128].T.astype(BF16)
    back = y_copies(Y_OUT, lambda p: out_send.at[:, pl.ds(pl.multiple_of(p * 32, 32), 32), :],
                    mine(out_recv))
    y_start(back)
    out_recv[y] = out_send[:, pl.ds(pl.multiple_of(y * 32, 32), 32), :]
    y_arrived(back)
    for i in range(NY):
        out[:, :, 128 * i:128 * i + 128] = out_recv[i]

    for w in idx_waits + [up_done, down_done] + coarse_waits + fine_waits:
        w.wait_send()
    for j in range(1, NZ):
        column_copy(j).wait_send()
    for g in range(NZ // 4):
        plane_all(g).wait_send()
    for copies in [feat_copies, down_copies, coarse_around, fine_around, back] + gather + merge + later:
        for c in copies:
            c.wait_send()


def per_device(features, fine_links, coarse_links, parents, down_weight, coarse_weight, up_weight,
               fine_weight, coarse_bias, fine_bias):
    y = lax.axis_index("chan")
    blank = lambda n: jnp.full((n,), -1, jnp.int32)
    link_rows = jnp.concatenate([
        fine_links.reshape(-1), blank(24), coarse_links.reshape(-1), parents, blank(72)])
    link_rows = link_rows.reshape(2, 1, 128)
    rows = lax.dynamic_index_in_dim(jnp.asarray(row_tables()), y, 0, keepdims=False)
    bias = jnp.stack([coarse_bias, fine_bias])
    bias = lax.dynamic_update_slice(jnp.zeros((8, 128), F32), bias, (0, y * 32))
    args = (
        link_rows, features, link_rows,
        jnp.transpose(down_weight, (0, 2, 1)), up_weight, coarse_weight, fine_weight, bias,
        jnp.broadcast_to(rows[:, None], (ROWS, 128)),
    )
    v = pltpu.VMEM
    scratch = dict(
        notes=v((2, 1, 128), jnp.int32), table=pltpu.SMEM((2, 1, 128), jnp.int32), asks=v((144, 1, 128), jnp.int32),
        idx_smem=pltpu.SMEM((144, 1, 128), jnp.int32), unfold=v((128, 128), BF16),
        octant=v((64, 64), BF16), coarse_pick=v((HALO, 256), BF16), fine_pick=v((HALO, 256), BF16),
        coarse_inner=v((1440, 512), BF16), coarse_outer=v((1440, 4 * HALO), BF16),
        fine_inner=v((960, 512), BF16), fine_outer=v((960, 4 * HALO), BF16),
        coarse_w_flat=v((128, 3456), BF16), fine_w_flat=v((128, 3456), BF16),
        il_recv=v((128, 1, 128), jnp.int32), ir_recv=v((128, 1, 128), jnp.int32),
        feats=v((4, 128, 128), BF16), down_all=v((4, 8, 32, 128), BF16), bias_all=v((4, 8, 128), F32),
        up_all=v((4, 8, 32, 128), BF16), coarse_w_all=v((4, 27, 32, 128), BF16),
        fine_w_all=v((4, 27, 32, 128), BF16), own=v((4, 128, 128), BF16), child=v((4, 16, 128), BF16),
        column=v((16, 4, 16, 128), BF16), relay_send=v((8, 16, 16, 128), BF16),
        up_recv=v((8, 16, 16, 128), BF16),
        coarse_all=v((4, 2, 128, 128), BF16), faces=v((24, 16, 128), BF16), rims=v((80, 2, 128), BF16),
        cf_send=v((128, 16, 128), BF16), cr_send=v((128, 2, 128), BF16),
        cf_recv=v((129, 16, 128), BF16), cr_recv=v((129, 2, 128), BF16),
        coarse_halo=v((4, 2, HALO, 128), BF16), frame=v((4, 1440, 128), F32),
        columns=v((512, 3456), BF16), octants=v((16, 16, 128), BF16),
        down_send=v((8, 16, 16, 128), BF16), down_mid=v((8, 16, 16, 128), BF16),
        down_out=v((16, 4, 16, 128), BF16), down_recv=v((16, 4, 16, 128), BF16),
        merged_all=v((4, 4, 128, 128), BF16),
        ff_send=v((128, 16, 128), BF16), fr_send=v((128, 2, 128), BF16),
        ff_recv=v((129, 16, 128), BF16), fr_recv=v((129, 2, 128), BF16),
        fine_halo=v((4, 4, HALO, 128), BF16), rim_rows=v((4, 48, 128), F32),
        out_send=v((4, 128, 128), BF16), out_recv=v((4, 4, 32, 128), BF16),
        y_ss=pltpu.SemaphoreType.DMA((13, 3)), y_rs=pltpu.SemaphoreType.DMA((13, 3)),
        b_ss=pltpu.SemaphoreType.DMA((8,)), b_rs=pltpu.SemaphoreType.DMA((8,)),
        a_ss=pltpu.SemaphoreType.DMA((16,)), a_rs=pltpu.SemaphoreType.DMA((16,)),
        d_ss=pltpu.SemaphoreType.DMA((4,)), d_rs=pltpu.SemaphoreType.DMA((4,)),
        local_sem=pltpu.SemaphoreType.DMA,
    )
    return pl.pallas_call(
        kernel,
        out_shape=jax.ShapeDtypeStruct((4, 32, 512), BF16),
        in_specs=[pl.BlockSpec(memory_space=pltpu.SMEM)] + [pl.BlockSpec(memory_space=v)] * 8,
        out_specs=pl.BlockSpec(memory_space=v),
        scratch_shapes=list(scratch.values()),
        compiler_params=pltpu.CompilerParams(collective_id=0, has_side_effects=True),
    )(*args)


def solution(mesh):
    in_specs = (
        P("brick", "chan", None), P("brick", None), P("brick", None), P("brick"),
        P(None, None, "chan"), P(None, "chan", None), P(None, "chan", None), P(None, "chan", None),
        P("chan"), P("chan"),
    )
    return jax.shard_map(
        per_device, mesh=mesh, in_specs=in_specs, out_specs=P("brick", "chan", None), check_vma=False
    )
```

```python
import functools

import jax
import jax.numpy as jnp
import numpy as np
from jax import lax
from jax.experimental import pallas as pl
from jax.experimental.pallas import tpu as pltpu
from jax.sharding import PartitionSpec as P

EDGE = 8
NX, NZ, NC = 4, 16, 2
PEERS = NX * NZ * NC
NY = 4
HALO = 144
MESH = pl.DeviceIdType.MESH
BF16 = jnp.bfloat16
F32 = jnp.float32


def headings():
    faces = [(1, 0, 0), (-1, 0, 0), (0, 1, 0), (0, -1, 0), (0, 0, 1), (0, 0, -1)]
    steps = [(a, b, c) for a in (-1, 0, 1) for b in (-1, 0, 1) for c in (-1, 0, 1)]
    return faces + [d for d in steps if sum(map(abs, d)) >= 2]


NUMBER = {d: k for k, d in enumerate(headings())}


def inner_row(fine, cell):
    if fine:
        low = [c // 2 for c in cell]
        part = [c % 2 for c in cell]
    else:
        low = [c % 4 for c in cell]
        part = [c // 4 for c in cell]
    return low[0], (4 * part[0] + 2 * part[1] + part[2]) * 16 + low[1] * 4 + low[2]


def halo_row(fine, d, cell):
    k = NUMBER[d]
    free = [cell[n] for n in range(3) if d[n] == 0]
    if not free:
        return 0, 96 + 2 * (k - 6)
    if d[0] == 0 and not fine:
        quarter, half = free[0] % 4, free[0] // 4
    else:
        quarter, half = free[0] // 2, free[0] % 2
    if len(free) == 2:
        return quarter, 16 * k + half * 8 + free[1]
    return quarter, 96 + 2 * (k - 6) + half


def frame_planes(fine, j):
    return [2 * j + n for n in range(4)] if fine else [j, j + 1, j + 2, j + 4, j + 5, j + 6]


def frame_tables(fine):
    inner, outer = [], []
    for j in range(NY):
        rows_in, rows_out = [], []
        for a3 in range(3):
            for px in frame_planes(fine, j):
                for py in range(10):
                    for z in range(8):
                        at = (px, py, z + a3)
                        d = tuple(1 if v == 9 else -1 if v == 0 else 0 for v in at)
                        cell = tuple(v - 1 for v in at)
                        if d == (0, 0, 0):
                            q, r = inner_row(fine, cell)
                            rows_in.append(q * 128 + r)
                            rows_out.append(-1)
                        else:
                            q, r = halo_row(fine, d, cell)
                            rows_in.append(-1)
                            rows_out.append(q * HALO + r)
        inner.append(rows_in)
        outer.append(rows_out)
    return np.array(inner, np.int32), np.array(outer, np.int32)


def piece_tables(fine):
    table = np.full((NY, HALO), -1, np.int32)
    for d in headings():
        edge = [0 if v == 1 else 7 for v in d]
        spans = [range(8) if v == 0 else (e,) for v, e in zip(d, edge)]
        for x in spans[0]:
            for y in spans[1]:
                for z in spans[2]:
                    cell = (x, y, z)
                    quarter, row = halo_row(fine, d, cell)
                    q, r = inner_row(fine, cell)
                    if x == 0:
                        table[quarter, row] = r
                    elif x == 7:
                        table[quarter, row] = r
                    else:
                        assert q == quarter
                        table[quarter, row] = 128 + r
    return table


def unfold_table():
    rows = []
    for o in range(8):
        for u in range(16):
            x, y, z = o // 4, 2 * (u // 4) + (o // 2) % 2, 2 * (u % 4) + o % 2
            rows.append(x * 64 + y * 8 + z)
    return np.array(rows, np.int32)


def octant_table():
    rows = []
    for q in range(4):
        for u in range(16):
            rows.append((4 * (q // 2) + u // 4) * 8 + 4 * (q % 2) + u % 4)
    return np.array(rows, np.int32)


def row_tables():
    unfold = np.broadcast_to(unfold_table(), (NY, 128))
    octant = np.broadcast_to(octant_table(), (NY, 64))
    frames = []
    for fine in (False, True):
        inner, outer = frame_tables(fine)
        frames.append(np.where(inner >= 0, inner, 512 + outer))
    return np.concatenate(
        [unfold, octant, piece_tables(False), piece_tables(True), frames[0], frames[1]], axis=1)


ROW_UNFOLD, ROW_OCTANT, ROW_CP, ROW_FP, ROW_CF, ROW_FF, ROWS = 0, 128, 192, 336, 480, 1920, 2880


AT_PAR = 52

Y_FEAT, Y_DOWN, Y_BIAS, Y_UP, Y_CW, Y_FW, Y_CG, Y_CG2, Y_CH, Y_CR, Y_MG, Y_MG2, Y_FH, Y_FR, Y_OUT = range(15)
B_IDX, B_IDR, B_UP, B_CF, B_CR, B_DOWN, B_FF, B_FR = range(8)


def nt(a, b):
    return lax.dot_general(a, b, (((1,), (1,)), ((), ())), preferred_element_type=F32)


def nn(a, b):
    return jnp.dot(a, b, preferred_element_type=F32)


def within(index, count):
    return jnp.minimum(jnp.maximum(index, 0), count - 1)


def choose(values, index):
    picked = values[0]
    for n in range(1, len(values)):
        picked = jnp.where(index == n, values[n], picked)
    return picked


def kernel(
    links, feat, link_rows, down_w, up_w, coarse_w, fine_w, bias, row_of,
    out,
    notes, table, asks, idx_smem, unfold, octant, coarse_pick, fine_pick, coarse_inner, coarse_outer,
    fine_inner, fine_outer, coarse_w_flat, fine_w_flat,
    il_recv, ir_recv, feats, down_all, bias_all, up_all, coarse_w_all, fine_w_all,
    own, child, column, relay_send, up_recv, coarse_all, faces, rims, cf_send, cr_send, cf_recv, cr_recv,
    coarse_halo, frame, columns, octants, down_send, down_mid, down_out, down_recv, merged_all, ff_send, fr_send,
    ff_recv, fr_recv, fine_halo, rim_rows, out_send, out_recv,
    y_ss, y_rs, b_ss, b_rs, a_ss, a_rs, d_ss, d_rs, local_sem,
):
    me, y = lax.axis_index("brick"), lax.axis_index("chan")
    x, z, core = me // (NZ * NC), me // NC % NZ, me % NC

    near = [(x + n // 2) % NX * (NZ * NC) + (core + n % 2) % NC for n in range(8)]

    def z_base(j):
        step = (j + 1) // 2
        ahead = z + step
        back = z + NZ - j // 2
        at = (j % 2) * ahead + (1 - j % 2) * back
        return at % NZ * NC

    def pick(dst, first, base, width):
        for at in range(0, width, 128):
            w = min(128, width - at)
            lanes = lax.broadcasted_iota(jnp.int32, (dst.shape[0], w), 1) + (base + at)
            hit = row_of[first:first + dst.shape[0], 0:w] == lanes
            dst[:, at:at + w] = jnp.where(hit, 1.0, 0.0).astype(BF16)

    barrier = pltpu.get_barrier_semaphore()

    def greet(j, base, first):
        for n in range(first, 8):
            pl.semaphore_signal(barrier, inc=1, device_id={"brick": near[n] + base}, device_id_type=MESH)

    def greet_far(t, carry):
        greet(15 - t, z_base(15 - t), 0)
        return carry

    lax.fori_loop(0, 15, greet_far, 0)
    greet(0, z * NC, 1)
    for k in range(1, NY):
        pl.semaphore_signal(barrier, inc=1, device_id={"chan": (y + k) % NY}, device_id_type=MESH)

    def slots(l, owner):
        dx, dz, dc = (x - (owner >> 5)) & 3, (z - (owner >> 1)) & 15, (core - owner) & 1
        j = jnp.where(dz == 0, 0, jnp.where(dz <= 8, 2 * dz - 1, 32 - 2 * dz))
        return j, jnp.where(l >= 0, j * 8 + dx * 2 + dc, PEERS)

    lane = lax.broadcasted_iota(jnp.int32, (1, 128), 1)
    fine_row, coarse_row = link_rows[0], link_rows[1]
    _, notes[0] = slots(fine_row, fine_row >> 2)
    j, slot = slots(coarse_row, jnp.where(lane < AT_PAR, coarse_row >> 1, coarse_row >> 4))
    notes[1] = jnp.where(lane < AT_PAR, slot, j)
    to_table = pltpu.make_async_copy(notes, table, local_sem)
    to_table.start()
    to_table.wait()
    pick(unfold, ROW_UNFOLD, 0, 128)
    pl.semaphore_wait(barrier, PEERS - 1 + NY - 1)

    def y_copies(phase, src, dst):
        return [
            pltpu.make_async_remote_copy(
                src_ref=src((y + k) % NY), dst_ref=dst, send_sem=y_ss.at[phase, k - 1],
                recv_sem=y_rs.at[phase, k - 1], device_id={"chan": (y + k) % NY}, device_id_type=MESH,
            )
            for k in range(1, NY)
        ]

    def y_start(copies):
        for c in copies:
            c.start()

    def y_arrived(copies):
        for c in copies:
            c.wait_recv()

    def b_all(phase, src, dst):
        return pltpu.make_async_remote_copy(
            src_ref=src.at[pl.ds(1, PEERS - 1)], dst_ref=dst.at[pl.ds(1, PEERS - 1)],
            send_sem=b_ss.at[phase], recv_sem=b_rs.at[phase],
            device_id={"brick": near[1] + z * NC}, device_id_type=MESH,
        )

    def send_group(exchanges, j, base, first):
        for n in range(first, 8):
            for phase, src, dst in exchanges:
                pltpu.make_async_remote_copy(
                    src_ref=src(8 * j + n), dst_ref=dst.at[8 * j + n], send_sem=b_ss.at[phase],
                    recv_sem=b_rs.at[phase], device_id={"brick": near[n] + base}, device_id_type=MESH,
                ).start()

    def exchange(exchanges, fill=None):
        def group(t, carry):
            if fill is not None:
                fill(14 - t, 14 - t + (t % 2) * 2 - 1 + jnp.where(t == 14, 1, 0))
            send_group(exchanges, 15 - t, z_base(15 - t), 0)
            return carry

        if fill is not None:
            fill(15, 15)
        lax.fori_loop(0, 15, group, 0)
        send_group(exchanges, 0, z * NC, 1)

    def mine(ref):
        return ref.at[y]

    feat_copies = y_copies(Y_FEAT, lambda p: feat.at[:, :, pl.ds(pl.multiple_of(p * 128, 128), 128)],
                           feats.at[:, pl.ds(pl.multiple_of(y * 32, 32), 32), :])
    y_start(feat_copies)
    down_copies = y_copies(Y_DOWN, lambda p: down_w, mine(down_all))
    y_start(down_copies)
    exchange(((B_IDX, lambda s: link_rows.at[0], il_recv), (B_IDR, lambda s: link_rows.at[1], ir_recv)))
    later = []

    def gather_weights(*weights):
        for phase, src, dst in weights:
            copies = y_copies(phase, lambda p, src=src: src, mine(dst))
            y_start(copies)
            later.append(copies)

    gather_weights((Y_BIAS, bias, bias_all), (Y_CW, coarse_w, coarse_w_all))
    feats[:, pl.ds(pl.multiple_of(y * 32, 32), 32), :] = (
        feat[:, :, pl.ds(pl.multiple_of(y * 128, 128), 128)])
    down_all[y] = down_w[...]
    bias_all[y] = bias[...]
    coarse_w_all[y] = coarse_w[...]
    up_all[y] = up_w[...]
    fine_w_all[y] = fine_w[...]
    il_recv[0] = link_rows[0]
    ir_recv[0] = link_rows[1]

    y_arrived(feat_copies)
    y_arrived(down_copies)
    for b in range(4):
        own[b] = nt(unfold[...], feats[b]).astype(BF16)
    total = jnp.zeros((64, 128), F32)
    for o in range(8):
        rows = jnp.concatenate([own[b, 16 * o:16 * o + 16, :] for b in range(4)], axis=0)
        weight = jnp.concatenate([down_all[i, o] for i in range(NY)], axis=0)
        total = total + nn(rows, weight)
    child[...] = total.astype(BF16).reshape(4, 16, 128)

    def column_copy(j):
        return pltpu.make_async_remote_copy(
            src_ref=child, dst_ref=column.at[j], send_sem=a_ss.at[j], recv_sem=a_rs.at[j],
            device_id={"brick": near[0] + z_base(j)}, device_id_type=MESH,
        )

    for j in range(1, NZ):
        column_copy(j).start()
    column[0] = child[...]

    zero = jnp.zeros((16, 128), BF16)
    for ref in (cf_recv, ff_recv):
        ref[PEERS] = zero
    for ref in (cr_recv, fr_recv):
        ref[PEERS] = jnp.zeros((2, 128), BF16)
    rim_rows[...] = jnp.zeros(rim_rows.shape, F32)

    pick(octant, ROW_OCTANT, 0, 64)
    pick(coarse_pick, ROW_CP, 0, 256)
    pick(coarse_inner, ROW_CF, 0, 512)
    pick(coarse_outer, ROW_CF, 512, 4 * HALO)

    idx_waits = [b_all(B_IDX, il_recv, il_recv), b_all(B_IDR, ir_recv, ir_recv)]
    for w in idx_waits:
        w.wait_recv()

    at = lax.broadcasted_iota(jnp.int32, (1, 1, 128), 2)

    k = at
    for n in (104, 78, 52, 26):
        k = jnp.where(at >= n, jnp.minimum(k, at - n), k)
    face, coarse, parent = k < 6, at < AT_PAR, (at >= AT_PAR) & (at < AT_PAR + 4)
    seen = il_recv[...]
    place_in = jnp.where(face, (seen & 3) * 6 + k, (seen & 3) * 20 + (k - 6))
    fine_ask = jnp.where((seen >> 2 == me) & (at < 104), place_in, 0)
    seen = ir_recv[...]
    place_in = jnp.where(face, (seen & 1) * 6 + k, (seen & 1) * 20 + (k - 6))
    coarse_ask = jnp.where((seen >> 1 == me) & coarse, place_in, 0)
    code_ask = jnp.where((seen >> 4 == me) & parent, (seen & 15) + 1, 0)
    total_asks = jnp.zeros((PEERS, 1, 128), jnp.int32)
    for field, v in enumerate((
            jnp.where(face, fine_ask, 0), jnp.where(face, 0, fine_ask),
            jnp.where(face, coarse_ask, 0), jnp.where(face, 0, coarse_ask), code_ask)):
        got = jnp.max(v, axis=2, keepdims=True)
        total_asks = jnp.where(at == field, got - (1 if field == 4 else 0), total_asks)
    asks[0:PEERS] = total_asks
    seen = jnp.concatenate([ir_recv[8 * j:8 * j + 1] for j in range(NZ)], axis=0)
    sent = jnp.zeros((NZ, 1, 128), jnp.int32)
    for n in range(8):
        v = jnp.where((seen >> 4 == near[n] + z * NC) & parent, at - AT_PAR, 0)
        got = jnp.max(v, axis=2, keepdims=True)
        sent = jnp.where(at == n, got, sent)
    asks[PEERS:PEERS + NZ] = jnp.where(
        parent, ((x - (seen >> 9)) & 3) * 2 + ((core - (seen >> 4)) & 1), sent)
    to_smem = pltpu.make_async_copy(asks, idx_smem, local_sem)
    to_smem.start()
    to_smem.wait()

    def relay_copy(n, g):
        return pltpu.make_async_remote_copy(
            src_ref=relay_send.at[n, pl.ds(4 * g, 4)], dst_ref=up_recv.at[n, pl.ds(4 * g, 4)],
            send_sem=b_ss.at[B_UP], recv_sem=b_rs.at[B_UP],
            device_id={"brick": near[n] + z * NC}, device_id_type=MESH,
        )

    for g in range(NZ // 4):
        for j in range(4 * g, 4 * g + 4):
            if j:
                column_copy(j).wait_recv()
        for j in range(4 * g, 4 * g + 4):
            children = [column[j, b] for b in range(4)]
            up_recv[0, j] = choose(children, idx_smem[PEERS + j, 0, 0])
            for n in range(1, 8):
                relay_send[n, j] = choose(children, idx_smem[PEERS + j, 0, n])
        for n in range(1, 8):
            relay_copy(n, g).start()

    up_done = pltpu.make_async_remote_copy(
        src_ref=relay_send.at[pl.ds(1, 7)], dst_ref=up_recv.at[pl.ds(1, 7)],
        send_sem=b_ss.at[B_UP], recv_sem=b_rs.at[B_UP],
        device_id={"brick": near[1] + z * NC}, device_id_type=MESH,
    )
    up_done.wait_recv()
    row = lax.broadcasted_iota(jnp.int32, (256, 128), 0)
    lane = lax.broadcasted_iota(jnp.int32, (256, 128), 1)
    same = row % 16 == lane % 16
    wide = lax.broadcasted_iota(jnp.int32, (1, 128), 1) // 16

    def add_children(g, acc):
        codes = jnp.zeros((1, 128), jnp.int32)
        for i in range(8):
            codes = jnp.where(wide == i, idx_smem[8 * (g % 2 * 8 + i) + g // 2, 0, 4], codes)
        hot = jnp.where(same & (row // 16 == codes), 1.0, 0.0).astype(BF16)
        return acc + nn(hot, up_recv[g // 2, pl.ds(g % 2 * 8, 8)].reshape(128, 128))

    summed = lax.fori_loop(0, PEERS // 8, add_children, jnp.zeros((256, 128), F32))
    coarse_all[y] = summed.astype(BF16).reshape(2, 128, 128)

    def in_halves(ref, first, second):
        copies = []
        for phase, half in ((first, y // 3), (second, 1 - y // 3)):
            part = ref.at[y, :, pl.ds(pl.multiple_of(64 * half, 64), 64), :]
            copies.append(y_copies(phase, lambda p, part=part: part, part))
            y_start(copies[-1])
        y_arrived(copies[0])
        return copies

    gather = in_halves(coarse_all, Y_CG, Y_CG2)
    gather_weights((Y_UP, up_w, up_all), (Y_FW, fine_w, fine_w_all))

    def halo(bricks, whole, pieces, f_field, link_row, f_phase, r_phase, y_phase,
             f_send, r_send, f_recv, r_recv, halo_all, inner, outer, rows, halves, meanwhile):
        for b in range(bricks):
            source = jnp.concatenate(
                [whole[0, b, 0:64, :], whole[NY - 1, b, 64:128, :], whole[y, b]], axis=0)
            found = nn(pieces[...], source)
            faces[pl.ds(6 * b, 6)] = found[:96].astype(BF16).reshape(6, 16, 128)
            for r in range(20):
                rims[20 * b + r] = found[96 + 2 * r:98 + 2 * r].astype(BF16)

        def answer(j, back):
            for n in range(8):
                asker = 8 * back + (NX - n // 2) % NX * 2 + n % 2
                f_send[8 * j + n] = faces[within(idx_smem[asker, 0, f_field], 6 * bricks)]
                r_send[8 * j + n] = rims[within(idx_smem[asker, 0, f_field + 1], 20 * bricks)]

        exchange(((f_phase, lambda s: f_send.at[s], f_recv), (r_phase, lambda s: r_send.at[s], r_recv)),
                 answer)
        f_recv[0] = f_send[0]
        r_recv[0] = r_send[0]
        meanwhile()
        y_arrived(halves[1])
        for b in range(bricks):
            source = jnp.concatenate([whole[i, b] for i in range(NY)], axis=0)
            frame[b, 0:rows, :] = nn(inner[...], source)
        waits = [b_all(f_phase, f_send, f_recv), b_all(r_phase, r_send, r_recv)]
        face_part, rim_part = halo_all.at[y, :, 0:96, :], halo_all.at[y, :, 96:HALO, :]
        waits[0].wait_recv()
        for b in range(bricks):
            for k in range(6):
                slot = within(table[link_row, 0, 26 * b + k], PEERS + 1)
                halo_all[y, b, 16 * k:16 * k + 16, :] = f_recv[slot]
        around = y_copies(y_phase, lambda p: face_part, face_part)
        y_start(around)
        waits[1].wait_recv()
        for b in range(bricks):
            for r in range(20):
                slot = within(table[link_row, 0, 26 * b + 6 + r], PEERS + 1)
                rim_rows[b, 2 * r:2 * r + 2, :] = r_recv[slot].astype(F32)
            halo_all[y, b, 96:HALO, :] = rim_rows[b].astype(BF16)
        rims_around = y_copies(y_phase + 1, lambda p: rim_part, rim_part)
        y_start(rims_around)
        around = around + rims_around
        y_arrived(around)
        for b in range(bricks):
            source = jnp.concatenate([halo_all[i, b] for i in range(NY)], axis=0)
            frame[b, 0:rows, :] = frame[b, 0:rows, :] + nn(outer[...], source)
        return waits, around

    def conv(bricks, planes, starts, weights, bias_row):
        for tap in range(27):
            a, a2, a3 = tap // 9, (tap // 3) % 3, tap % 3
            for b in range(bricks):
                for n, start in enumerate(starts):
                    at = ((a3 * planes + start + a) * 10 + a2) * 8
                    columns[(2 * b + n) * 64:(2 * b + n + 1) * 64, tap * 128:tap * 128 + 128] = (
                        frame[b, at:at + 64, :].astype(BF16))
        whole = nt(columns[0:bricks * 128, :], weights[...])
        shift = bias_all[0] + bias_all[1] + bias_all[2] + bias_all[3]
        return jnp.maximum(whole + shift[bias_row:bias_row + 1, :], 0.0)

    def flatten_weights():
        for copies in later:
            y_arrived(copies)
        for tap in range(27):
            for i in range(NY):
                for src, dst in ((coarse_w_all, coarse_w_flat), (fine_w_all, fine_w_flat)):
                    dst[32 * i:32 * i + 32, tap * 128:tap * 128 + 128] = src[i, tap]
        pick(fine_pick, ROW_FP, 0, 256)
        pick(fine_inner, ROW_FF, 0, 512)
        pick(fine_outer, ROW_FF, 512, 4 * HALO)

    coarse_waits, coarse_around = halo(
        2, coarse_all, coarse_pick, 2, 1, B_CF, B_CR, Y_CH,
        cf_send, cr_send, cf_recv, cr_recv, coarse_halo, coarse_inner, coarse_outer, 1440,
        gather, flatten_weights)
    coarse_out = conv(2, 6, (0, 3), coarse_w_flat, 0).astype(BF16)
    for p in range(2):
        for n in range(2):
            at = (2 * p + n) * 64
            octants[pl.ds(8 * p + 4 * n, 4)] = (
                nn(octant[...], coarse_out[at:at + 64]).astype(BF16).reshape(4, 16, 128))

    def plane_copy(n, g):
        return pltpu.make_async_remote_copy(
            src_ref=down_send.at[n, pl.ds(4 * g, 4)], dst_ref=down_mid.at[n, pl.ds(4 * g, 4)],
            send_sem=d_ss.at[g], recv_sem=d_rs.at[g],
            device_id={"brick": near[n] + z * NC}, device_id_type=MESH,
        )

    def plane_all(g):
        return pltpu.make_async_remote_copy(
            src_ref=down_send.at[pl.ds(1, 7), pl.ds(4 * g, 4)],
            dst_ref=down_mid.at[pl.ds(1, 7), pl.ds(4 * g, 4)],
            send_sem=d_ss.at[g], recv_sem=d_rs.at[g],
            device_id={"brick": near[1] + z * NC}, device_id_type=MESH,
        )

    def back_of(j):
        return j if j in (0, NZ - 1) else j + 1 if j % 2 else j - 1

    for g in range(NZ // 4 - 1, -1, -1):
        for j in range(4 * g, 4 * g + 4):
            for n in range(8):
                asker = 8 * back_of(j) + (NX - n // 2) % NX * 2 + n % 2
                found = octants[within(idx_smem[asker, 0, 4], 16)]
                if n:
                    down_send[n, j] = found
                else:
                    down_mid[0, j] = found
        for n in range(1, 8):
            plane_copy(n, g).start()
    for g in range(NZ // 4 - 1, -1, -1):
        plane_all(g).wait_recv()
        for j in range(4 * g, 4 * g + 4):
            arrived = [down_mid[n, j] for n in range(8)]
            for b in range(4):
                down_out[j, b] = choose(arrived, idx_smem[PEERS + back_of(j), 0, AT_PAR + b])
        for j in range(4 * g + 3, 4 * g - 1, -1):
            if j:
                pltpu.make_async_remote_copy(
                    src_ref=down_out.at[j], dst_ref=down_recv.at[j], send_sem=b_ss.at[B_DOWN],
                    recv_sem=b_rs.at[B_DOWN], device_id={"brick": near[0] + z_base(j)},
                    device_id_type=MESH,
                ).start()
    down_recv[0] = down_out[0]
    down_done = pltpu.make_async_remote_copy(
        src_ref=down_out.at[pl.ds(1, NZ - 1)], dst_ref=down_recv.at[pl.ds(1, NZ - 1)],
        send_sem=b_ss.at[B_DOWN], recv_sem=b_rs.at[B_DOWN],
        device_id={"brick": near[0] + z_base(1)}, device_id_type=MESH,
    )
    down_done.wait_recv()
    coarse_rows = jnp.concatenate([down_recv[within(table[1, 0, AT_PAR + b], NZ), b] for b in range(4)], axis=0)
    for o in range(8):
        weight = jnp.concatenate([up_all[i, o] for i in range(NY)], axis=0)
        lifted = nt(coarse_rows, weight)
        for b in range(4):
            merged_all[y, b, 16 * o:16 * o + 16, :] = (
                own[b, 16 * o:16 * o + 16, :].astype(F32) + lifted[16 * b:16 * b + 16]).astype(BF16)
    merge = in_halves(merged_all, Y_MG, Y_MG2)

    fine_waits, fine_around = halo(
        4, merged_all, fine_pick, 0, 0, B_FF, B_FR, Y_FH,
        ff_send, fr_send, ff_recv, fr_recv, fine_halo, fine_inner, fine_outer, 960,
        merge, lambda: None)
    refined = conv(4, 4, (0, 1), fine_w_flat, 1)
    for b in range(4):
        out_send[b] = refined[128 * b:128 * b + 128].T.astype(BF16)
    back = y_copies(Y_OUT, lambda p: out_send.at[:, pl.ds(pl.multiple_of(p * 32, 32), 32), :],
                    mine(out_recv))
    y_start(back)
    out_recv[y] = out_send[:, pl.ds(pl.multiple_of(y * 32, 32), 32), :]
    y_arrived(back)
    for i in range(NY):
        out[:, :, 128 * i:128 * i + 128] = out_recv[i]

    for w in idx_waits + [up_done, down_done] + coarse_waits + fine_waits:
        w.wait_send()
    for j in range(1, NZ):
        column_copy(j).wait_send()
    for g in range(NZ // 4):
        plane_all(g).wait_send()
    for copies in [feat_copies, down_copies, coarse_around, fine_around, back] + gather + merge + later:
        for c in copies:
            c.wait_send()


def per_device(features, fine_links, coarse_links, parents, down_weight, coarse_weight, up_weight,
               fine_weight, coarse_bias, fine_bias):
    y = lax.axis_index("chan")
    blank = lambda n: jnp.full((n,), -1, jnp.int32)
    link_rows = jnp.concatenate([
        fine_links.reshape(-1), blank(24), coarse_links.reshape(-1), parents, blank(72)])
    link_rows = link_rows.reshape(2, 1, 128)
    rows = lax.dynamic_index_in_dim(jnp.asarray(row_tables()), y, 0, keepdims=False)
    bias = jnp.stack([coarse_bias, fine_bias])
    bias = lax.dynamic_update_slice(jnp.zeros((8, 128), F32), bias, (0, y * 32))
    args = (
        link_rows, features, link_rows,
        jnp.transpose(down_weight, (0, 2, 1)), up_weight, coarse_weight, fine_weight, bias,
        jnp.broadcast_to(rows[:, None], (ROWS, 128)),
    )
    v = pltpu.VMEM
    scratch = dict(
        notes=v((2, 1, 128), jnp.int32), table=pltpu.SMEM((2, 1, 128), jnp.int32), asks=v((144, 1, 128), jnp.int32),
        idx_smem=pltpu.SMEM((144, 1, 128), jnp.int32), unfold=v((128, 128), BF16),
        octant=v((64, 64), BF16), coarse_pick=v((HALO, 256), BF16), fine_pick=v((HALO, 256), BF16),
        coarse_inner=v((1440, 512), BF16), coarse_outer=v((1440, 4 * HALO), BF16),
        fine_inner=v((960, 512), BF16), fine_outer=v((960, 4 * HALO), BF16),
        coarse_w_flat=v((128, 3456), BF16), fine_w_flat=v((128, 3456), BF16),
        il_recv=v((128, 1, 128), jnp.int32), ir_recv=v((128, 1, 128), jnp.int32),
        feats=v((4, 128, 128), BF16), down_all=v((4, 8, 32, 128), BF16), bias_all=v((4, 8, 128), F32),
        up_all=v((4, 8, 32, 128), BF16), coarse_w_all=v((4, 27, 32, 128), BF16),
        fine_w_all=v((4, 27, 32, 128), BF16), own=v((4, 128, 128), BF16), child=v((4, 16, 128), BF16),
        column=v((16, 4, 16, 128), BF16), relay_send=v((8, 16, 16, 128), BF16),
        up_recv=v((8, 16, 16, 128), BF16),
        coarse_all=v((4, 2, 128, 128), BF16), faces=v((24, 16, 128), BF16), rims=v((80, 2, 128), BF16),
        cf_send=v((128, 16, 128), BF16), cr_send=v((128, 2, 128), BF16),
        cf_recv=v((129, 16, 128), BF16), cr_recv=v((129, 2, 128), BF16),
        coarse_halo=v((4, 2, HALO, 128), BF16), frame=v((4, 1440, 128), F32),
        columns=v((512, 3456), BF16), octants=v((16, 16, 128), BF16),
        down_send=v((8, 16, 16, 128), BF16), down_mid=v((8, 16, 16, 128), BF16),
        down_out=v((16, 4, 16, 128), BF16), down_recv=v((16, 4, 16, 128), BF16),
        merged_all=v((4, 4, 128, 128), BF16),
        ff_send=v((128, 16, 128), BF16), fr_send=v((128, 2, 128), BF16),
        ff_recv=v((129, 16, 128), BF16), fr_recv=v((129, 2, 128), BF16),
        fine_halo=v((4, 4, HALO, 128), BF16), rim_rows=v((4, 48, 128), F32),
        out_send=v((4, 128, 128), BF16), out_recv=v((4, 4, 32, 128), BF16),
        y_ss=pltpu.SemaphoreType.DMA((15, 3)), y_rs=pltpu.SemaphoreType.DMA((15, 3)),
        b_ss=pltpu.SemaphoreType.DMA((8,)), b_rs=pltpu.SemaphoreType.DMA((8,)),
        a_ss=pltpu.SemaphoreType.DMA((16,)), a_rs=pltpu.SemaphoreType.DMA((16,)),
        d_ss=pltpu.SemaphoreType.DMA((4,)), d_rs=pltpu.SemaphoreType.DMA((4,)),
        local_sem=pltpu.SemaphoreType.DMA,
    )
    return pl.pallas_call(
        kernel,
        out_shape=jax.ShapeDtypeStruct((4, 32, 512), BF16),
        in_specs=[pl.BlockSpec(memory_space=pltpu.SMEM)] + [pl.BlockSpec(memory_space=v)] * 8,
        out_specs=pl.BlockSpec(memory_space=v),
        scratch_shapes=list(scratch.values()),
        compiler_params=pltpu.CompilerParams(collective_id=0, has_side_effects=True),
    )(*args)


def solution(mesh):
    in_specs = (
        P("brick", "chan", None), P("brick", None), P("brick", None), P("brick"),
        P(None, None, "chan"), P(None, "chan", None), P(None, "chan", None), P(None, "chan", None),
        P("chan"), P("chan"),
    )
    return jax.shard_map(
        per_device, mesh=mesh, in_specs=in_specs, out_specs=P("brick", "chan", None), check_vma=False
    )
```
